32 devices in a mesh: dp: 8 (over z, x), mp: 4 (over y, core).
Axes of the slice: x: 2, y: 2, z: 4, core: 2. Of those that a mesh axis runs over, the one named last changes fastest.
Arguments:
- tokens: bfloat16 [8192, 2048], P(('dp', 'mp')), may hold values from -12 to 12
- cotangent: float32 [8192, 2048], P(('dp', 'mp')), may hold values from -6 to 6
- segments: int32 [8192], P('dp'), may hold values from -1 to 7679, as said below
- positions: int32 [8192], P('dp'), may hold values from 0 to 511, as said below
- step_count: int32 [1], replicated, may hold values from 1 to 20
- w_heads_in: bfloat16 [3, 2048, 2048], P(None, 'dp', 'mp'), may hold values from -0.44194174 to 0.44194174
- first_heads_in: float32 [3, 2048, 2048], P(None, 'dp', 'mp'), may hold values from -96 to 96
- second_heads_in: float32 [3, 2048, 2048], P(None, 'dp', 'mp'), may hold values from 200 to 5000
- w_heads_out: bfloat16 [2048, 2048], P('dp', 'mp'), may hold values from -0.125 to 0.125
- first_heads_out: float32 [2048, 2048], P('dp', 'mp'), may hold values from -96 to 96
- second_heads_out: float32 [2048, 2048], P('dp', 'mp'), may hold values from 200 to 5000
- w_gate_up: bfloat16 [2, 2048, 8192], P(None, 'dp', 'mp'), may hold values from -0.125 to 0.125
- first_gate_up: float32 [2, 2048, 8192], P(None, 'dp', 'mp'), may hold values from -96 to 96
- second_gate_up: float32 [2, 2048, 8192], P(None, 'dp', 'mp'), may hold values from 200 to 5000
- w_down: bfloat16 [2048, 8192], P('dp', 'mp'), may hold values from -0.0625 to 0.0625
- first_down: float32 [2048, 8192], P('dp', 'mp'), may hold values from -96 to 96
- second_down: float32 [2048, 8192], P('dp', 'mp'), may hold values from 200 to 5000
- gains: float32 [4, 2048], replicated, may hold values from 0.5 to 1.5
- first_gains: float32 [4, 2048], replicated, may hold values from -96 to 96
- second_gains: float32 [4, 2048], replicated, may hold values from 200 to 5000
Outputs:
- block_out: float32 [8192, 2048], P(('dp', 'mp'))
- input_grad: float32 [8192, 2048], P(('dp', 'mp'))
- grad_heads_in: float32 [3, 2048, 2048], P(None, 'dp', 'mp')
- new_first_heads_in: float32 [3, 2048, 2048], P(None, 'dp', 'mp')
- new_second_heads_in: float32 [3, 2048, 2048], P(None, 'dp', 'mp')
- update_heads_in: float32 [3, 2048, 2048], P(None, 'dp', 'mp')
- grad_heads_out: float32 [2048, 2048], P('dp', 'mp')
- new_first_heads_out: float32 [2048, 2048], P('dp', 'mp')
- new_second_heads_out: float32 [2048, 2048], P('dp', 'mp')
- update_heads_out: float32 [2048, 2048], P('dp', 'mp')
- grad_gate_up: float32 [2, 2048, 8192], P(None, 'dp', 'mp')
- new_first_gate_up: float32 [2, 2048, 8192], P(None, 'dp', 'mp')
- new_second_gate_up: float32 [2, 2048, 8192], P(None, 'dp', 'mp')
- update_gate_up: float32 [2, 2048, 8192], P(None, 'dp', 'mp')
- grad_down: float32 [2048, 8192], P('dp', 'mp')
- new_first_down: float32 [2048, 8192], P('dp', 'mp')
- new_second_down: float32 [2048, 8192], P('dp', 'mp')
- update_down: float32 [2048, 8192], P('dp', 'mp')
- grad_gains: float32 [4, 2048], replicated
- new_first_gains: float32 [4, 2048], replicated
- new_second_gains: float32 [4, 2048], replicated
- update_gains: float32 [4, 2048], replicated
The draws below stay inside these ranges and needn't reach their ends.
Inputs may be any that keep to these rules, and one draw needn't show every extreme that they name: `segments`: each group's 1024 slots hold whole sequences laid end to end in consecutive slots, each of 1 to 512 tokens, with ids unique in the batch; a sequence's id is the index of its first slot in the whole batch; at least the first 512 slots of every group are used, unused slots at a group's end carry -1; no sequence crosses a slot whose index in its group is a multiple of 512; the largest id is that of the last group's last sequence, of one token at that group's slot 511. `positions`: position of a slot within its sequence, counted from 0; 0 on unused slots.
All inputs are finite; a program needn't handle non-finite values.
Results may differ from the reference program's by a relative error of at most 0.017.
The reference program's roundings to bfloat16 on the way count: a program that leaves them out, or rounds other values in their place, can miss the bound.
Values may be sent and summed in bfloat16 or wider, within the bound.
A program may use at most 256 MiB of HBM per device.

```python
import math
import jax
import jax.numpy as jnp
from jax import lax

D = 2048
HEADS = 16
HEAD_DIM = 128
FF = 8192
MAXLEN = 512
GRP = 1024
TOKENS = 8192


def layout(key):
    key_base = jax.random.fold_in(key, 7)
    key_used, key_cut = jax.random.split(key_base)
    groups = TOKENS // GRP
    slot_index = jnp.arange(GRP, dtype=jnp.int32)
    group_index = jnp.arange(groups, dtype=jnp.int32)
    used_slots = jax.random.randint(key_used, (groups,), GRP // 2, GRP + 1, dtype=jnp.int32)
    used_slots = jnp.where(group_index == 0, GRP, used_slots)
    used_slots = jnp.where(group_index == groups - 1, GRP // 2, used_slots)
    odds = max(MAXLEN // 4, 2)
    boundary = jax.random.randint(key_cut, (groups, GRP), 0, odds, dtype=jnp.int32) == 0
    boundary = boundary | (slot_index % MAXLEN == 0)[None, :]
    last_cut = (group_index[:, None] == groups - 1) & (slot_index[None, :] == GRP // 2 - 1)
    boundary = boundary | last_cut
    first_long = (group_index[:, None] == 0) & (slot_index[None, :] < MAXLEN)
    boundary = jnp.where(first_long, (slot_index == 0)[None, :], boundary)
    seq_start = lax.cummax(jnp.where(boundary, slot_index[None, :], 0), axis=1)
    is_live = slot_index[None, :] < used_slots[:, None]
    segment_ids = jnp.where(is_live, group_index[:, None] * GRP + seq_start, -1)
    position_ids = jnp.where(is_live, slot_index[None, :] - seq_start, 0)
    return (segment_ids.reshape(-1).astype(jnp.int32), position_ids.reshape(-1).astype(jnp.int32))


def draw_segments(key, part):
    return layout(key)[0]


def draw_positions(key, part):
    return layout(key)[1]


def draw_tokens(key, part):
    key_base = jax.random.fold_in(key, 11)
    key_entry, key_scale = jax.random.split(key_base, 2)
    entries = jax.random.normal(key_entry, (TOKENS, D), jnp.float32)
    row_scale = jnp.exp(jax.random.uniform(key_scale, (TOKENS, 1), jnp.float32, math.log(0.4), math.log(4.0)))
    return jnp.clip(entries * row_scale, -12.0, 12.0).astype(jnp.bfloat16)


def draw_w_heads_in(key, part):
    key_base = jax.random.fold_in(key, 23)
    key_entry, key_scale = jax.random.split(key_base)
    trend = jnp.exp(jnp.arange(D, dtype=jnp.float32) * (math.log(3.0) / (D - 1)))
    spread = jnp.exp(jax.random.uniform(key_scale, (3, 1, D), jnp.float32, 0.0, math.log(3.3)))
    entries = jnp.clip(jax.random.normal(key_entry, (3, D, D), jnp.float32), -6.0, 6.0)
    return (entries * trend[None, None, :] * spread * (1.0 / (3.0 * math.sqrt(D)))).astype(jnp.bfloat16)


def levels(own_key, extent, shards, least, high):
    gain = 1.0
    for dim, shards_of in shards:
        heights = jax.random.uniform(jax.random.fold_in(jax.random.fold_in(own_key, 6), dim), (shards_of,), jnp.float32, least / len(shards), high / len(shards))
        gain = gain * jnp.repeat(jnp.exp(heights), extent[dim] // shards_of).reshape((-1,) + (1,) * (len(extent) - 1 - dim))
    return gain


def gaussian(own_key, dims, scale, limit, pieces=(), held_as=jnp.bfloat16):
    gain = levels(own_key, dims, pieces, -0.22, 0.18) if pieces else 1.0
    values = jax.random.normal(own_key, dims, jnp.float32) * scale * gain
    return jnp.minimum(jnp.maximum(values, -limit), limit).astype(held_as)


def setup_inputs(seed: int = 0) -> dict:
    splits = jax.random.split(jax.random.key(seed), 21)
    tokens = draw_tokens(jax.random.fold_in(splits[20], 71), 0)
    cotangent = gaussian(splits[1], (TOKENS, D), 1.0, 6.0, ((0, 32),), jnp.float32)
    segments = draw_segments(jax.random.fold_in(splits[20], 71), 0)
    positions = draw_positions(jax.random.fold_in(splits[20], 71), 0)
    step_count = jax.random.randint(splits[4], (1,), 1, 21).astype(jnp.int32)
    w_heads_in = draw_w_heads_in(jax.random.fold_in(splits[20], 71), 0)
    first_heads_in = gaussian(splits[6], (3, D, D), 15.0, 96.0, ((1, 8), (2, 4)), jnp.float32)
    second_heads_in = jnp.clip(jnp.exp(math.log(5000.0) - 3.218876 * jax.random.uniform(splits[7], (3, D, D), jnp.float32) ** levels(splits[7], (3, D, D), ((1, 8), (2, 4)), -0.2, 0.2)), 200.0, 5000.0)
    w_heads_out = gaussian(splits[8], (D, D), D ** -0.5, 0.125, ((0, 8), (1, 4)))
    first_heads_out = gaussian(splits[9], (D, D), 15.0, 96.0, ((0, 8), (1, 4)), jnp.float32)
    second_heads_out = jnp.clip(jnp.exp(math.log(5000.0) - 3.218876 * jax.random.uniform(splits[10], (D, D), jnp.float32) ** levels(splits[10], (D, D), ((0, 8), (1, 4)), -0.2, 0.2)), 200.0, 5000.0)
    w_gate_up = gaussian(splits[11], (2, D, FF), D ** -0.5, 0.125, ((1, 8), (2, 4)))
    first_gate_up = gaussian(splits[12], (2, D, FF), 15.0, 96.0, ((1, 8), (2, 4)), jnp.float32)
    second_gate_up = jnp.clip(jnp.exp(math.log(5000.0) - 3.218876 * jax.random.uniform(splits[13], (2, D, FF), jnp.float32) ** levels(splits[13], (2, D, FF), ((1, 8), (2, 4)), -0.2, 0.2)), 200.0, 5000.0)
    w_down = gaussian(splits[14], (D, FF), FF ** -0.5, 0.0625, ((0, 8), (1, 4)))
    first_down = gaussian(splits[15], (D, FF), 15.0, 96.0, ((0, 8), (1, 4)), jnp.float32)
    second_down = jnp.clip(jnp.exp(math.log(5000.0) - 3.218876 * jax.random.uniform(splits[16], (D, FF), jnp.float32) ** levels(splits[16], (D, FF), ((0, 8), (1, 4)), -0.2, 0.2)), 200.0, 5000.0)
    gains = jnp.clip(1.0 + 0.1 * jax.random.normal(splits[17], (4, D), jnp.float32), 0.5, 1.5)
    first_gains = gaussian(splits[18], (4, D), 15.0, 96.0, (), jnp.float32)
    second_gains = jnp.clip(jnp.exp(jax.random.uniform(splits[19], (4, D), jnp.float32, math.log(200.0), math.log(5000.0))), 200.0, 5000.0)
    return dict(tokens=tokens, cotangent=cotangent, segments=segments, positions=positions, step_count=step_count, w_heads_in=w_heads_in, first_heads_in=first_heads_in, second_heads_in=second_heads_in, w_heads_out=w_heads_out, first_heads_out=first_heads_out, second_heads_out=second_heads_out, w_gate_up=w_gate_up, first_gate_up=first_gate_up, second_gate_up=second_gate_up, w_down=w_down, first_down=first_down, second_down=second_down, gains=gains, first_gains=first_gains, second_gains=second_gains)


EPS = 1e-06
THETA = 500000.0
NEG = -1e+30
BETA_ONE = 0.9
BETA_TWO = 0.95
ADAM_EPS = 1e-08
RATE = 0.03
DECAY = 0.1
HIGH = lax.Precision.HIGHEST

@jax.custom_vjp
def low(v):
    return lax.optimization_barrier(v.astype(jnp.bfloat16)).astype(jnp.float32)

@jax.custom_vjp
def low_back(v):
    return v

def low_keep(v):
    return (low(v), None)

def low_pass(kept, grad):
    return (grad,)

def back_keep(v):
    return (v, None)

def back_low(kept, grad):
    return (low(grad),)
low.defvjp(low_keep, low_pass)
low_back.defvjp(back_keep, back_low)

def product(left, right):
    return jnp.dot(left, right, precision=HIGH)

def rotation(positions, head_dim):
    half = head_dim // 2
    freq = THETA ** (-jnp.arange(half, dtype=jnp.float32) * 2.0 / head_dim)
    angle = positions.astype(jnp.float32)[:, None] * freq[None, :]
    angle = jnp.concatenate([angle, angle], axis=1)
    return (jnp.cos(angle), jnp.sin(angle))

def turn_half(values):
    half = values.shape[-1] // 2
    return jnp.concatenate([-values[..., half:], values[..., :half]], axis=-1)

def rotate(values, cosine, sine):
    return values * cosine[:, None, :] + turn_half(values) * sine[:, None, :]

def attention(q_rot, k_rot, v_low, segment):
    group_rows = q_rot.shape[0]
    block_rows = min(512, group_rows)
    count_blocks = group_rows // block_rows
    score_scale = HEAD_DIM ** (-0.5)
    slot_index = jnp.arange(group_rows, dtype=jnp.int32)

    def one_block(block_index):
        first_row = (block_index * block_rows).astype(jnp.int32)
        q_block = lax.dynamic_slice_in_dim(q_rot, first_row, block_rows, 0)
        scores = jnp.einsum('qhd,khd->hqk', q_block, k_rot, precision=HIGH) * score_scale
        scores = low_back(scores)
        row_slots = first_row + jnp.arange(block_rows, dtype=jnp.int32)
        row_segments = lax.dynamic_slice_in_dim(segment, first_row, block_rows, 0)
        allowed = (row_segments[:, None] == segment[None, :]) & (slot_index[None, :] <= row_slots[:, None])
        scores = jnp.where(allowed[None], scores, NEG)
        highest = lax.optimization_barrier(jnp.max(scores, axis=-1, keepdims=True))
        weights = jnp.exp(scores - highest)
        prob_block = low(weights / lax.optimization_barrier(jnp.sum(weights, axis=-1, keepdims=True)))
        return jnp.einsum('hqk,khd->qhd', prob_block, v_low, precision=HIGH)
    result = lax.map(jax.checkpoint(one_block), jnp.arange(count_blocks, dtype=jnp.int32))
    return result.reshape(group_rows, -1)

def layer_group(x_rows, segment, position, heads_in, heads_out, gate_up, down_weight, gain_rows):
    group_rows = x_rows.shape[0]
    queries = low_back(product(x_rows, heads_in[0]))
    keys_raw = low_back(product(x_rows, heads_in[1]))
    values = low_back(product(x_rows, heads_in[2]))
    q_hat = queries * lax.rsqrt(lax.optimization_barrier(jnp.mean(queries * queries, axis=1, keepdims=True)) + EPS)
    k_hat = keys_raw * lax.rsqrt(lax.optimization_barrier(jnp.mean(keys_raw * keys_raw, axis=1, keepdims=True)) + EPS)
    cosine, sine = rotation(position, HEAD_DIM)
    q_rot = low(rotate((q_hat * gain_rows[0]).reshape(group_rows, HEADS, HEAD_DIM), cosine, sine))
    k_rot = low(rotate((k_hat * gain_rows[1]).reshape(group_rows, HEADS, HEAD_DIM), cosine, sine))
    v_low = low(values).reshape(group_rows, HEADS, HEAD_DIM)
    attended = low_back(low(attention(q_rot, k_rot, v_low, segment)))
    branch = low_back(product(attended, heads_out.T))
    a_hat = branch * lax.rsqrt(lax.optimization_barrier(jnp.mean(branch * branch, axis=1, keepdims=True)) + EPS)
    hidden = x_rows + a_hat * gain_rows[2]
    hidden_low = low(hidden)
    gate_values = low_back(product(hidden_low, gate_up[0]))
    up_values = low_back(product(hidden_low, gate_up[1]))
    hidden_act = low(jax.nn.silu(gate_values) * up_values)
    mlp_branch = low_back(product(hidden_act, down_weight.T))
    m_hat = mlp_branch * lax.rsqrt(lax.optimization_barrier(jnp.mean(mlp_branch * mlp_branch, axis=1, keepdims=True)) + EPS)
    return hidden + m_hat * gain_rows[3]

def adamw_step(weight, grad, first, second, decay, fix_one, fix_two):
    first_new = BETA_ONE * first + (1.0 - BETA_ONE) * grad
    second_new = BETA_TWO * second + (1.0 - BETA_TWO) * grad * grad
    step_size = first_new / fix_one / (jnp.sqrt(second_new / fix_two) + ADAM_EPS) + decay * weight
    return (first_new, second_new, -RATE * step_size)

def reference(tokens, cotangent, segments, positions, step_count, w_heads_in, first_heads_in, second_heads_in, w_heads_out, first_heads_out, second_heads_out, w_gate_up, first_gate_up, second_gate_up, w_down, first_down, second_down, gains, first_gains, second_gains):
    groups = tokens.shape[0] // GRP
    seg_groups = segments.reshape(groups, GRP)
    pos_groups = positions.reshape(groups, GRP)

    def forward(x_all, heads_in, heads_out, gate_up, down_weight, gain_rows):

        def one_group(items):
            return layer_group(items[0], items[1], items[2], heads_in, heads_out, gate_up, down_weight, gain_rows)
        result = lax.map(one_group, (x_all.reshape(groups, GRP, -1), seg_groups, pos_groups))
        return result.reshape(x_all.shape)
    x_all = tokens.astype(jnp.float32)
    heads_in = w_heads_in.astype(jnp.float32)
    heads_out = w_heads_out.astype(jnp.float32)
    gate_up = w_gate_up.astype(jnp.float32)
    down_weight = w_down.astype(jnp.float32)
    gain_rows = gains.astype(jnp.float32)
    block_out, pullback = jax.vjp(forward, x_all, heads_in, heads_out, gate_up, down_weight, gain_rows)
    input_grad, grad_heads_in, grad_heads_out, grad_gate_up, grad_down, grad_gains = pullback(cotangent.astype(jnp.float32))
    step_float = step_count[0].astype(jnp.float32)
    fix_one = 1.0 - jnp.exp(step_float * jnp.log(jnp.float32(BETA_ONE)))
    fix_two = 1.0 - jnp.exp(step_float * jnp.log(jnp.float32(BETA_TWO)))
    f_in, s_in, u_in = adamw_step(heads_in, grad_heads_in, first_heads_in, second_heads_in, DECAY, fix_one, fix_two)
    f_out, s_out, u_out = adamw_step(heads_out, grad_heads_out, first_heads_out, second_heads_out, DECAY, fix_one, fix_two)
    f_gu, s_gu, u_gu = adamw_step(gate_up, grad_gate_up, first_gate_up, second_gate_up, DECAY, fix_one, fix_two)
    f_down, s_down, u_down = adamw_step(down_weight, grad_down, first_down, second_down, DECAY, fix_one, fix_two)
    f_gain, s_gain, u_gain = adamw_step(gain_rows, grad_gains, first_gains, second_gains, 0.0, fix_one, fix_two)
    return (block_out, input_grad, grad_heads_in, f_in, s_in, u_in, grad_heads_out, f_out, s_out, u_out, grad_gate_up, f_gu, s_gu, u_gu, grad_down, f_down, s_down, u_down, grad_gains, f_gain, s_gain, u_gain)
```

```python
import functools

import jax
import jax.numpy as jnp
from jax import lax
from jax.experimental import pallas as pl
from jax.experimental.pallas import tpu as pltpu
from jax.sharding import PartitionSpec as P

HEAD_DIM = 128
HALF = 512
EPS = 1e-06
THETA = 500000.0
NEG = -1e30
BETA_ONE = 0.9
BETA_TWO = 0.95
ADAM_EPS = 1e-08
RATE = 0.03
DECAY = 0.1

F32 = jnp.float32
BF16 = jnp.bfloat16


def mm(left, right):
    return jnp.dot(left, right, preferred_element_type=F32)


def mm_nt(left, right):
    return lax.dot_general(left, right, (((1,), (1,)), ((), ())), preferred_element_type=F32)


def mm_tn(left, right):
    return lax.dot_general(left, right, (((0,), (0,)), ((), ())), preferred_element_type=F32)


def forward_kernel(
    q_ref, k_ref, v_ref, rq_ref, rk_ref, gq_ref, gk_ref, cos_ref, sin_ref,
    seg_q_ref, seg_k_ref, slot_q_ref, slot_k_ref,
    qr_ref, kr_ref, vl_ref, out_ref, lse_ref, bias_ref,
):
    @pl.when(pl.program_id(1) == 0)
    def _():
        allowed = (seg_q_ref[...] == seg_k_ref[...]) & (slot_k_ref[...] <= slot_q_ref[...])
        bias_ref[...] = jnp.where(allowed, 0.0, NEG)

    cosine, sine = cos_ref[...], sin_ref[...]

    def rotated(raw, recip, gain):
        normed = raw * recip * gain
        return (normed * cosine + pltpu.roll(normed, HEAD_DIM // 2, 1) * sine).astype(BF16)

    q_rot = rotated(q_ref[...], rq_ref[...], gq_ref[...])
    k_rot = rotated(k_ref[...], rk_ref[...], gk_ref[...])
    v_low = v_ref[...].astype(BF16)
    qr_ref[...] = q_rot
    kr_ref[...] = k_rot
    vl_ref[...] = v_low
    scores = mm_nt(q_rot, k_rot) * (HEAD_DIM**-0.5) + bias_ref[...]
    highest = jnp.max(scores, axis=1, keepdims=True)
    weights = jnp.exp(scores - highest)
    total = jnp.sum(weights, axis=1, keepdims=True)
    probs = (weights / total).astype(BF16)
    out_ref[...] = mm(probs, v_low).astype(BF16)
    lse_ref[...] = jnp.broadcast_to(highest + jnp.log(total), lse_ref.shape)


def backward_kernel(
    qr_ref, kr_ref, vl_ref, do_ref, lse_ref, q_ref, k_ref, rq_ref, rk_ref, gq_ref, gk_ref,
    cos_ref, sin_ref, seg_q_ref, seg_k_ref, slot_q_ref, slot_k_ref,
    eq_ref, ek_ref, dv_ref, sum_q_ref, sum_k_ref, gain_q_ref, gain_k_ref, bias_ref,
):
    head = pl.program_id(1)

    @pl.when(head == 0)
    def _():
        allowed = (seg_q_ref[...] == seg_k_ref[...]) & (slot_k_ref[...] <= slot_q_ref[...])
        bias_ref[...] = jnp.where(allowed, 0.0, NEG)
        sum_q_ref[...] = jnp.zeros_like(sum_q_ref)
        sum_k_ref[...] = jnp.zeros_like(sum_k_ref)

    scale = HEAD_DIM**-0.5
    q_rot, k_rot, grad_out = qr_ref[...], kr_ref[...], do_ref[...]
    scores = mm_nt(q_rot, k_rot) * scale + bias_ref[...]
    probs = jnp.exp(scores - lse_ref[:, :1])
    grad_probs = mm_nt(grad_out, vl_ref[...])
    delta = jnp.sum(grad_probs * probs, axis=1, keepdims=True)
    grad_scores = (probs * (grad_probs - delta)).astype(BF16)
    dv_ref[...] = mm_tn(probs.astype(BF16), grad_out).astype(BF16)
    cosine, sine = cos_ref[...], sin_ref[...]

    def back(grad_rot, raw_ref, recip_ref, gain_ref, e_ref, sum_ref, gain_out_ref):
        grad = grad_rot * cosine - pltpu.roll(grad_rot, HEAD_DIM // 2, 1) * sine
        hat = raw_ref[...] * recip_ref[...]
        gain_out_ref[...] = jnp.sum((grad * hat).reshape(-1, 8, HEAD_DIM), axis=0)
        scaled = grad * gain_ref[...]
        e_ref[...] = scaled
        sum_ref[...] += jnp.sum(scaled * hat, axis=1, keepdims=True)

    back(mm(grad_scores, k_rot) * scale, q_ref, rq_ref, gq_ref, eq_ref, sum_q_ref, gain_q_ref)
    back(mm_tn(grad_scores, q_rot) * scale, k_ref, rk_ref, gk_ref, ek_ref, sum_k_ref, gain_k_ref)


def attention_specs():
    tile = pl.BlockSpec((HALF, HEAD_DIM), lambda i, h: (i, h))
    column = pl.BlockSpec((HALF, 1), lambda i, h: (i, 0))
    lane = pl.BlockSpec((1, HALF), lambda i, h: (0, i))
    gain = pl.BlockSpec((1, HEAD_DIM), lambda i, h: (0, h))
    trig = pl.BlockSpec((HALF, HEAD_DIM), lambda i, h: (i, 0))
    return tile, column, lane, gain, trig


def attend(q, k, v, recip_q, recip_k, gain_q, gain_k, cosine, sine, seg, slot):
    rows, columns = q.shape
    heads = columns // HEAD_DIM
    tile, column, lane, gain, trig = attention_specs()
    low = jax.ShapeDtypeStruct((rows, columns), BF16)
    return pl.pallas_call(
        forward_kernel,
        grid=(rows // HALF, heads),
        in_specs=[tile, tile, tile, column, column, gain, gain, trig, trig, column, lane, column, lane],
        out_specs=[tile] * 5,
        out_shape=[low, low, low, low, jax.ShapeDtypeStruct((rows, columns), F32)],
        scratch_shapes=[pltpu.VMEM((HALF, HALF), F32)],
        name="attend_forward",
        cost_estimate=pl.CostEstimate(
            flops=4 * rows * HALF * columns,
            bytes_accessed=rows * columns * 24,
            transcendentals=rows * HALF * heads,
        ),
    )(
        q, k, v, recip_q, recip_k, gain_q, gain_k, cosine, sine,
        seg[:, None], seg[None, :], slot[:, None], slot[None, :],
    )


def attend_back(
    q_rot, k_rot, v_low, grad_out, lse, q, k, recip_q, recip_k, gain_q, gain_k, cosine, sine, seg, slot
):
    rows, columns = q.shape
    heads = columns // HEAD_DIM
    halves = rows // HALF
    tile, column, lane, gain, trig = attention_specs()
    wide = jax.ShapeDtypeStruct((rows, columns), F32)
    summed = jax.ShapeDtypeStruct((rows, 1), F32)
    parts = jax.ShapeDtypeStruct((8 * halves, columns), F32)
    return pl.pallas_call(
        backward_kernel,
        grid=(halves, heads),
        in_specs=[tile] * 7 + [column, column, gain, gain, trig, trig, column, lane, column, lane],
        out_specs=[tile, tile, tile, column, column]
        + [pl.BlockSpec((8, HEAD_DIM), lambda i, h: (i, h))] * 2,
        out_shape=[
            wide, wide, jax.ShapeDtypeStruct((rows, columns), BF16), summed, summed, parts, parts,
        ],
        scratch_shapes=[pltpu.VMEM((HALF, HALF), F32)],
        name="attend_backward",
        cost_estimate=pl.CostEstimate(
            flops=10 * rows * HALF * columns,
            bytes_accessed=rows * columns * 30,
            transcendentals=rows * HALF * heads,
        ),
    )(
        q_rot, k_rot, v_low, grad_out, lse, q, k, recip_q, recip_k, gain_q, gain_k, cosine, sine,
        seg[:, None], seg[None, :], slot[:, None], slot[None, :],
    )


def ring_of(count):
    return list(range(0, count, 2)) + list(range(count - 1, 0, -2))


class Ring:
    def __init__(self, count):
        self.count, self.half = count, count // 2
        order = ring_of(count)
        self.order = order
        self.up = [(order[i], order[(i + 1) % count]) for i in range(count)]
        self.down = [(b, a) for a, b in self.up]
        place = [0] * count
        for i, owner in enumerate(order):
            place[owner] = i
        self.place = place

    def send_up(self, value):
        return lax.ppermute(value, "dp", self.up)

    def send_down(self, value):
        return lax.ppermute(value, "dp", self.down)

    def gather(self, first, second):
        n, h = self.count, self.half
        one, two = {0: first}, {0: second}
        a, b, c, d = first, second, first, second
        for step in range(1, h + 1):
            a = self.send_up(a)
            one[n - step] = a
            d = self.send_down(d)
            two[step] = d
            if step < h:
                b = self.send_up(b)
                two[n - step] = b
                c = self.send_down(c)
                one[step] = c
        return [(one[k], two[k]) for k in range(n)]

    def reduce(self, term):
        n, h = self.count, self.half
        a = term(0, h).astype(BF16)
        d = term(1, h).astype(BF16)
        b = c = None
        for step in range(1, h + 1):
            a, d = self.send_up(a), self.send_down(d)
            if step > 1:
                b, c = self.send_up(b), self.send_down(c)
            k = h - step
            if k == 0:
                break
            a = (term(0, k) + a).astype(BF16)
            d = (term(1, n - k) + d).astype(BF16)
            two, one = term(1, k), term(0, n - k)
            b = (two if b is None else two + b).astype(BF16)
            c = (one if c is None else one + c).astype(BF16)
        return term(0, 0) + a + c, term(1, 0) + d + b

    def rotate(self, values, place):
        width = values.shape[-1] // self.count
        pieces = [values[..., i * width : (i + 1) * width] for i in self.order]
        twice = jnp.concatenate(pieces + pieces, axis=-1)
        return lax.dynamic_slice_in_dim(twice, place * width, values.shape[-1], values.ndim - 1)

    def unrotate(self, values, place):
        width = values.shape[-1] // self.count
        twice = jnp.concatenate([values, values], axis=-1)
        start = lax.rem(self.count - place, self.count) * width
        ordered = lax.dynamic_slice_in_dim(twice, start, values.shape[-1], values.ndim - 1)
        return jnp.concatenate(
            [ordered[..., i * width : (i + 1) * width] for i in self.place], axis=-1
        )


class Cube:
    def __init__(self, count):
        self.count = count
        self.bits = [1 << i for i in range(count.bit_length() - 1)]

    def swap(self, value, bit, axis="mp", count=None):
        count = count or self.count
        return lax.ppermute(value, axis, [(i, i ^ bit) for i in range(count)])

    def gather(self, value):
        blocks = {0: value}
        for bit in reversed(self.bits):
            for r, block in list(blocks.items()):
                blocks[r ^ bit] = self.swap(block, bit)
        return [blocks[r] for r in range(self.count)]

    def scatter(self, block):
        held = {r: block(r) for r in reversed(range(self.count))}
        for bit in self.bits:
            last = bit == self.bits[-1]
            kept = {}
            for r in sorted(held, reverse=True):
                if r & bit:
                    got = self.swap(held[r], bit)
                    total = held[r ^ bit].astype(F32) + got
                    kept[r ^ bit] = total if last else total.astype(BF16)
            held = kept
        return held[0]

    def total(self, value):
        for bit in self.bits:
            got = self.swap(value, bit)
            order = [r ^ bit for r in range(self.count)]
            value = value + jnp.stack([got[:, r] for r in order], axis=1)
        return value


def adamw_step(weight, grad, first, second, decay, fix_one, fix_two):
    first_new = BETA_ONE * first + (1.0 - BETA_ONE) * grad
    second_new = BETA_TWO * second + (1.0 - BETA_TWO) * grad * grad
    step_size = first_new / fix_one / (
        jnp.sqrt(second_new / fix_two) + ADAM_EPS
    ) + decay * weight.astype(F32)
    return (first_new, second_new, -RATE * step_size)


def body(
    dp, mp,
    tokens, cotangent, segments, positions, step_count,
    w_heads_in, first_heads_in, second_heads_in,
    w_heads_out, first_heads_out, second_heads_out,
    w_gate_up, first_gate_up, second_gate_up,
    w_down, first_down, second_down,
    gains, first_gains, second_gains,
):
    ring, cube = Ring(dp), Cube(mp)
    n = dp
    own_rows, width = tokens.shape
    rows = own_rows * mp
    block = width // n
    columns = w_heads_in.shape[2]
    hidden_columns = w_down.shape[1]
    mp_index = lax.axis_index("mp")
    dp_index = lax.axis_index("dp")
    place = jnp.take(jnp.array(ring.place, jnp.int32), dp_index)
    row_block = [mp_index ^ r for r in range(mp)]

    half_block = block // 2
    in_blocks = ring.gather(w_heads_in[:, :half_block], w_heads_in[:, half_block:])
    out_blocks = ring.gather(w_heads_out[:half_block], w_heads_out[half_block:])
    gate_up_blocks = ring.gather(w_gate_up[0], w_gate_up[1])
    down_blocks = ring.gather(w_down[:half_block], w_down[half_block:])

    def xor_rows(values):
        return jnp.concatenate(
            [lax.dynamic_slice_in_dim(values, b * own_rows, own_rows, 0) for b in row_block]
        )

    seg = xor_rows(segments)
    pos = xor_rows(positions)
    slot = jnp.concatenate([b * own_rows + jnp.arange(own_rows, dtype=jnp.int32) for b in row_block])
    half_dim = HEAD_DIM // 2
    freq = THETA ** (-jnp.arange(half_dim, dtype=F32) * 2.0 / HEAD_DIM)
    angle = pos.astype(F32)[:, None] * freq[None, :]
    cos_half, sin_half = jnp.cos(angle), jnp.sin(angle)
    cosine = jnp.concatenate([cos_half, cos_half], axis=1)
    sine = jnp.concatenate([-sin_half, sin_half], axis=1)

    x_low = ring.rotate(tokens, place)
    cot = ring.rotate(cotangent, place)
    gains_model = ring.rotate(gains[2:4], place)
    gain_attn, gain_mlp = gains_model[0:1], gains_model[1:2]
    gain_heads = lax.dynamic_slice_in_dim(gains[0:2], mp_index * columns, columns, 1)
    gain_q, gain_k = gain_heads[0:1], gain_heads[1:2]

    x_full = jnp.concatenate(cube.gather(x_low))
    heads_in = jnp.concatenate([piece for pair in in_blocks for piece in pair], axis=1)
    q = mm(x_full, heads_in[0])
    k = mm(x_full, heads_in[1])
    v = mm(x_full, heads_in[2])
    squares = jnp.stack([jnp.sum(q * q, axis=1), jnp.sum(k * k, axis=1)])
    squares = cube.total(squares.reshape(2, mp, own_rows)).reshape(2, rows)
    recip = lax.rsqrt(squares / width + EPS)
    recip_q, recip_k = recip[0][:, None], recip[1][:, None]
    q_rot, k_rot, v_low, attended, lse = attend(
        q, k, v, recip_q, recip_k, gain_q, gain_k, cosine, sine, seg, slot
    )

    def row_part(values, r):
        return values[r * own_rows : (r + 1) * own_rows]

    heads_out = jnp.concatenate([piece for pair in out_blocks for piece in pair], axis=0)
    branch_terms = mm_nt(attended, heads_out).astype(BF16)
    branch = cube.scatter(lambda r: row_part(branch_terms, r))
    recip_a = lax.rsqrt(jnp.mean(branch * branch, axis=1, keepdims=True) + EPS)
    a_hat = branch * recip_a
    hidden = x_low.astype(F32) + a_hat * gain_attn
    hidden_full = jnp.concatenate(cube.gather(hidden.astype(BF16)))

    gate_up = [jnp.concatenate([pair[i] for pair in gate_up_blocks], axis=0) for i in range(2)]
    gate = mm(hidden_full, gate_up[0])
    up = mm(hidden_full, gate_up[1])
    sigmoid = jax.nn.sigmoid(gate)
    silu = gate * sigmoid
    act = (silu * up).astype(BF16)

    far = [[ring.half]] + [[s, n - s] for s in range(ring.half - 1, 0, -1)] + [[0]]
    groups = [far[0], far[1], sum(far[2:-1], []) + far[-1]]

    def by_group(make):
        found = {}
        for group in reversed(groups):
            whole = make(group)
            for i, b in enumerate(group):
                found[b] = whole[:, i * block : (i + 1) * block]
        return found

    def down_group(group):
        weight = jnp.concatenate([piece for b in group for piece in down_blocks[b]], axis=0)
        terms = mm_nt(act, weight).astype(BF16)
        return cube.scatter(lambda r: row_part(terms, r))

    mlp_parts = by_group(down_group)
    mlp = jnp.concatenate([mlp_parts[b] for b in range(n)], axis=1)
    recip_m = lax.rsqrt(jnp.mean(mlp * mlp, axis=1, keepdims=True) + EPS)
    m_hat = mlp * recip_m
    block_out = hidden + m_hat * gain_mlp
    gain_post_mlp = jnp.sum(cot * m_hat, axis=0)
    dy_mlp = cot * gain_mlp
    grad_mlp = (
        recip_m * (dy_mlp - m_hat * jnp.mean(dy_mlp * m_hat, axis=1, keepdims=True))
    ).astype(BF16)
    grad_mlp_blocks = {}
    for group in groups:
        own = jnp.concatenate([grad_mlp[:, b * block : (b + 1) * block] for b in group], axis=1)
        whole = jnp.concatenate(cube.gather(own))
        for i, b in enumerate(group):
            grad_mlp_blocks[b] = whole[:, i * block : (i + 1) * block]

    half_columns = hidden_columns // 2
    act_halves = (act[:, :half_columns], act[:, half_columns:])
    grad_down = jnp.concatenate(
        ring.reduce(lambda i, b: mm_tn(grad_mlp_blocks[b], act_halves[i])), axis=1
    )

    down_full = jnp.concatenate([piece for pair in down_blocks for piece in pair], axis=0)
    grad_mlp_full = jnp.concatenate([grad_mlp_blocks[b] for b in range(n)], axis=1)
    grad_act = mm(grad_mlp_full, down_full)
    grad_gate = (grad_act * up * sigmoid * (1.0 + gate * (1.0 - sigmoid))).astype(BF16)
    grad_up = (grad_act * silu).astype(BF16)
    grad_gate_up_halves = (grad_gate, grad_up)
    grad_gate_up = jnp.stack(
        ring.reduce(
            lambda i, b: mm_tn(
                hidden_full[:, b * block : (b + 1) * block], grad_gate_up_halves[i]
            )
        )
    )
    hidden_terms = (mm_nt(grad_gate, gate_up[0]) + mm_nt(grad_up, gate_up[1])).astype(BF16)
    grad_hidden = cot + cube.scatter(lambda r: row_part(hidden_terms, r))

    gain_post_attn = jnp.sum(grad_hidden * a_hat, axis=0)
    dy_attn = grad_hidden * gain_attn
    grad_branch = (
        recip_a * (dy_attn - a_hat * jnp.mean(dy_attn * a_hat, axis=1, keepdims=True))
    ).astype(BF16)
    grad_branch_full = jnp.concatenate(cube.gather(grad_branch))
    grad_attended = mm(grad_branch_full, heads_out).astype(BF16)
    out_half = columns // 2
    attended_halves = (attended[:, :out_half], attended[:, out_half:])
    grad_heads_out = jnp.concatenate(
        ring.reduce(
            lambda i, b: mm_tn(
                grad_branch_full[:, b * block : (b + 1) * block], attended_halves[i]
            )
        ),
        axis=1,
    )
    scaled_q, scaled_k, grad_v, sum_q, sum_k, gain_q_parts, gain_k_parts = attend_back(
        q_rot, k_rot, v_low, grad_attended, lse, q, k, recip_q, recip_k, gain_q, gain_k,
        cosine, sine, seg, slot,
    )
    back_sums = jnp.stack([sum_q[:, 0], sum_k[:, 0]]).reshape(2, mp, own_rows)
    back_sums = cube.total(back_sums).reshape(2, rows) / width
    grad_q = (recip_q * (scaled_q - q * recip_q * back_sums[0][:, None])).astype(BF16)
    grad_k = (recip_k * (scaled_k - k * recip_k * back_sums[1][:, None])).astype(BF16)
    grad_proj = jnp.concatenate([grad_q, grad_k, grad_v], axis=1)
    proj_half = 3 * columns // 2
    proj_halves = (grad_proj[:, :proj_half], grad_proj[:, proj_half:])
    grad_in = jnp.concatenate(
        ring.reduce(lambda i, b: mm_tn(x_full[:, b * block : (b + 1) * block], proj_halves[i])),
        axis=1,
    )
    grad_heads_in = jnp.stack([grad_in[:, c * columns : (c + 1) * columns] for c in range(3)])
    input_terms = (
        mm_nt(grad_q, heads_in[0]) + mm_nt(grad_k, heads_in[1]) + mm_nt(grad_v, heads_in[2])
    ).astype(BF16)
    input_grad = grad_hidden + cube.scatter(lambda r: row_part(input_terms, r))

    norm_parts = lax.dynamic_update_slice(
        jnp.zeros((2, width), F32),
        jnp.stack([jnp.sum(gain_q_parts, axis=0), jnp.sum(gain_k_parts, axis=0)]),
        (jnp.int32(0), mp_index * columns),
    )
    model_parts = ring.unrotate(jnp.stack([gain_post_attn, gain_post_mlp]), place)
    grad_gains = jnp.concatenate([norm_parts, model_parts])
    for bit in cube.bits:
        grad_gains = grad_gains + cube.swap(grad_gains, bit)
    for i in range(n.bit_length() - 1):
        grad_gains = grad_gains + cube.swap(grad_gains, 1 << i, "dp", n)

    step_float = step_count[0].astype(F32)
    fix_one = 1.0 - jnp.exp(step_float * jnp.log(F32(BETA_ONE)))
    fix_two = 1.0 - jnp.exp(step_float * jnp.log(F32(BETA_TWO)))
    outs = [ring.unrotate(block_out, place), ring.unrotate(input_grad, place)]
    for weight, grad, first, second, decay in (
        (w_heads_in, grad_heads_in, first_heads_in, second_heads_in, DECAY),
        (w_heads_out, grad_heads_out, first_heads_out, second_heads_out, DECAY),
        (w_gate_up, grad_gate_up, first_gate_up, second_gate_up, DECAY),
        (w_down, grad_down, first_down, second_down, DECAY),
        (gains, grad_gains, first_gains, second_gains, 0.0),
    ):
        outs.append(grad)
        outs.extend(adamw_step(weight, grad, first, second, decay, fix_one, fix_two))
    return tuple(outs)


def solution(mesh):
    rows = P(("dp", "mp"), None)
    stacked = P(None, "dp", "mp")
    flat = P("dp", "mp")
    in_specs = (
        (rows, rows, P("dp"), P("dp"), P())
        + (stacked,) * 3 + (flat,) * 3 + (stacked,) * 3 + (flat,) * 3 + (P(),) * 3
    )
    out_specs = (rows, rows) + (stacked,) * 4 + (flat,) * 4 + (stacked,) * 4 + (flat,) * 4 + (P(),) * 4
    step = functools.partial(body, mesh.shape["dp"], mesh.shape["mp"])
    return jax.shard_map(step, mesh=mesh, in_specs=in_specs, out_specs=out_specs, check_vma=False)
```
